32 devices in a mesh: dp: 2 (over x), tp: 4 (over z), cp: 4 (over y, core).
Axes of the slice: x: 2, y: 2, z: 4, core: 2. Of those that a mesh axis runs over, the one named last changes fastest.
Arguments:
- x_tokens: bfloat16 [24576, 2048], P(('dp', 'cp', 'tp')), parts along dimension 0
- w_q: bfloat16 [2048, 24, 128], P(None, 'tp')
- w_k: bfloat16 [2048, 24, 128], P(None, 'tp')
- w_v: bfloat16 [2048, 24, 128], P(None, 'tp')
- w_o: bfloat16 [24, 128, 2048], P('tp')
Outputs:
- output: bfloat16 [24576, 2048], P(('dp', 'cp', 'tp')), parts along dimension 0
There are 2 independent parts. The reference program is written for one: setup_inputs(seed, part) draws one part's arguments, and reference() takes and returns one part's arrays. A program takes and returns all parts, laid end to end along the dimension named above; an argument that names none is the same for every part.
All inputs are finite; a program needn't handle non-finite values.
Results may differ from the reference program's by a relative error of at most 0.00553008.
Values are sent between devices in bfloat16 or wider.
A program may use at most 1 GiB of HBM per device.

```python
import jax
import jax.numpy as jnp
from jax import lax

SEQ_LEN = 12288
CP_SIZE = 4
D_MODEL = 2048
NUM_HEADS = 24
HEAD_DIM = 128


def setup_inputs(seed: int = 0, part: int = 0) -> dict:
    root_key = jax.random.key(seed)
    x_key = jax.random.fold_in(jax.random.fold_in(root_key, 1), part)
    q_key, k_key, v_key, o_key = jax.random.split(jax.random.fold_in(root_key, 2), 4)
    in_scale = D_MODEL ** -0.5
    out_scale = (NUM_HEADS * HEAD_DIM) ** -0.5
    head_shape = (D_MODEL, NUM_HEADS, HEAD_DIM)
    x_tokens = jax.random.normal(x_key, (SEQ_LEN, D_MODEL), jnp.float32)
    w_q = jax.random.normal(q_key, head_shape, jnp.float32) * (2.5 * in_scale)
    w_k = jax.random.normal(k_key, head_shape, jnp.float32) * in_scale
    w_v = jax.random.normal(v_key, head_shape, jnp.float32) * in_scale
    w_o = jax.random.normal(o_key, (NUM_HEADS, HEAD_DIM, D_MODEL), jnp.float32) * out_scale
    return {'x_tokens': x_tokens.astype(jnp.bfloat16), 'w_q': w_q.astype(jnp.bfloat16), 'w_k': w_k.astype(jnp.bfloat16), 'w_v': w_v.astype(jnp.bfloat16), 'w_o': w_o.astype(jnp.bfloat16)}


def token_positions():
    shard_len = SEQ_LEN // CP_SIZE
    block_len = shard_len // 2
    token_idx = jnp.arange(SEQ_LEN, dtype=jnp.int32)
    owner_shard = token_idx // shard_len
    within = token_idx % shard_len
    nat_block = jnp.where(within < block_len, owner_shard, 2 * CP_SIZE - 1 - owner_shard)
    return nat_block * block_len + within % block_len


def reference(x_tokens, w_q, w_k, w_v, w_o):
    def project(weight):
        flat = jnp.dot(x_tokens, weight.reshape(D_MODEL, NUM_HEADS * HEAD_DIM), preferred_element_type=jnp.float32)
        return flat.astype(jnp.bfloat16).reshape(SEQ_LEN, NUM_HEADS, HEAD_DIM).transpose(1, 0, 2)

    q_heads = project(w_q)
    k_heads = project(w_k)
    v_heads = project(w_v)
    positions = token_positions()
    n_blocks = 2 * CP_SIZE
    block_len = SEQ_LEN // n_blocks
    inv_sqrt = HEAD_DIM ** -0.5

    def one_head(head_args):
        q_head, k_head, v_head = head_args

        def one_block(block_args):
            q_blk, q_pos = block_args
            scores = jnp.dot(q_blk, k_head.T, preferred_element_type=jnp.float32) * inv_sqrt
            causal_mask = positions[None, :] <= q_pos[:, None]
            scores = jnp.where(causal_mask, scores, -1e30)
            weights = jnp.exp(scores - scores.max(axis=-1, keepdims=True))
            row_total = weights.sum(axis=-1, keepdims=True)
            block_out = jnp.dot(weights.astype(jnp.bfloat16), v_head, preferred_element_type=jnp.float32) / row_total
            return block_out.astype(jnp.bfloat16)

        head_blocks = lax.map(one_block, (q_head.reshape(n_blocks, block_len, HEAD_DIM), positions.reshape(n_blocks, block_len)))
        return head_blocks.reshape(SEQ_LEN, HEAD_DIM)

    attn_heads = lax.map(one_head, (q_heads, k_heads, v_heads))
    attn_flat = attn_heads.transpose(1, 0, 2).reshape(SEQ_LEN, NUM_HEADS * HEAD_DIM)
    y_full = jnp.dot(attn_flat, w_o.reshape(NUM_HEADS * HEAD_DIM, D_MODEL), preferred_element_type=jnp.float32)
    return y_full.astype(jnp.bfloat16)
```

```python
import functools

import jax
import jax.numpy as jnp
import numpy as np
from jax import lax
from jax.experimental import pallas as pl
from jax.experimental.pallas import tpu as pltpu
from jax.sharding import PartitionSpec as P


LOG2E = 1.4426950408889634
ARRIVAL = ((0, 1, 2, 3), (1, 0, 2, 3), (2, 3, 1, 0), (3, 2, 1, 0))
HALF = 384
GROUPS = 3


def sub_block(run, rank, n_cp):
    if run < 2:
        return 2 * rank + run
    return 2 * (2 * n_cp - 1 - rank) + run - 2


LOCAL, REMOTE = (0, 1), (2, 3)


def key_slots(spec):
    return [4 * step + src for step, sources in spec for src in sources]


AVAIL = [
    key_slots([(0, LOCAL), (0, REMOTE), (1, LOCAL)]),
    key_slots([(0, LOCAL + REMOTE), (1, LOCAL + REMOTE), (2, LOCAL)]),
    key_slots([(0, LOCAL + REMOTE), (1, LOCAL + REMOTE), (2, LOCAL + REMOTE), (3, LOCAL)]),
    key_slots([(s, LOCAL + REMOTE) for s in range(4)]),
]
Q_SLOTS = [2, 3, 4, 4]
ROW = 20


def work_tables(n_tp, n_cp):
    def make(before, after):
        out = np.zeros((n_tp, n_cp, 5, ROW), np.int32)
        for z in range(n_tp):
            for r in range(n_cp):
                for i in range(Q_SLOTS[after]):
                    mine = sub_block(ARRIVAL[z][i], r, n_cp)
                    done = before >= 0 and i < Q_SLOTS[before]
                    keys = []
                    for j in AVAIL[after]:
                        if done and j in AVAIL[before]:
                            continue
                        other = sub_block(ARRIVAL[z][j // 4], r ^ (j % 4), n_cp)
                        if other < mine:
                            keys.append(j)
                    out[z, r, i, 0] = len(keys)
                    out[z, r, i, 1:1 + len(keys)] = keys
                order = (0, 1, 3, 2) if z in (1, 2) else (0, 1, 2, 3)
                out[z, r, 4, :4] = order
        return out.reshape(n_tp * n_cp, 5 * ROW)

    return make


def attend_kernel(cfg, tbl, *refs):
    (n_q, n_state, keys, final, rows, scale) = cfg
    refs = list(refs)
    q_in = [refs.pop(0) for _ in range(n_q)]
    kv_in = [refs.pop(0) for _ in keys]
    st_in = [[refs.pop(0) for _ in range(3)] for _ in range(n_state)]
    if final:
        o_out = [refs.pop(0) for _ in range(4)]
    else:
        st_out = [[refs.pop(0) for _ in range(3)] for _ in range(n_q)]
    q_scr, k_scr, v_scr, acc, m_scr, l_scr = refs
    hd = q_scr.shape[-1]

    def at(n):
        return pl.ds(n * rows, rows)

    for i in range(n_q):
        q_scr[at(i), :] = q_in[i][...]
    for j, ref in zip(keys, kv_in):
        k_scr[at(j), :] = ref[:, :hd]
        v_scr[at(j), :] = ref[:, hd:]
    for i in range(n_state):
        for dst, src in zip((acc, m_scr, l_scr), st_in[i]):
            dst[at(i), :] = src[...]

    def scores(q, kj, n):
        return lax.dot_general(q, k_scr[pl.ds(kj, n), :], (((1,), (1,)), ((), ())), preferred_element_type=jnp.float32)

    def lane_sums(p):
        out = p[:, :hd]
        for t in range(1, p.shape[1] // hd):
            out = out + p[:, t * hd:(t + 1) * hd]
        return out

    chunks = list(range(0, rows, HALF))

    for i in range(n_state, n_q):
        base = i * rows
        raws = [scores(q_scr[pl.ds(base + c, HALF), :], 4 * i * rows, c + HALF) for c in chunks]
        for c, s in zip(chunks, raws):
            n = c + HALF
            keep = lax.broadcasted_iota(jnp.int32, (HALF, n), 1) <= lax.broadcasted_iota(jnp.int32, (HALF, n), 0) + c
            s = jnp.where(keep, s * scale, -jnp.inf)
            m_new = jnp.broadcast_to(jnp.max(s, axis=1, keepdims=True), (HALF, hd))
            p = jnp.exp2(s - m_new[:, :1])
            here = pl.ds(base + c, HALF)
            l_scr[here, :] = lane_sums(p)
            m_scr[here, :] = m_new
            acc[here, :] = jnp.dot(p.astype(jnp.bfloat16), v_scr[pl.ds(4 * i * rows, n), :], preferred_element_type=jnp.float32)

    def update(base, kjs):
        def raw(c):
            q = q_scr[pl.ds(base + c, HALF), :]
            return [scores(q, kj, rows) for kj in kjs]

        nxt = raw(0)
        for n, c in enumerate(chunks):
            cur = nxt
            if n + 1 < len(chunks):
                nxt = raw(chunks[n + 1])
            here = pl.ds(base + c, HALF)
            m_old = m_scr[here, :]
            top = functools.reduce(jnp.maximum, cur)
            m_new = jnp.maximum(m_old, jnp.max(top, axis=1, keepdims=True) * scale)
            alpha = jnp.exp2(m_old - m_new)
            ps = [jnp.exp2(s * scale - m_new[:, :1]) for s in cur]
            sums = functools.reduce(jnp.add, [lane_sums(p) for p in ps])
            l_scr[here, :] = alpha * l_scr[here, :] + sums
            m_scr[here, :] = m_new
            pv = functools.reduce(jnp.add, [jnp.dot(p.astype(jnp.bfloat16), v_scr[pl.ds(kj, rows), :], preferred_element_type=jnp.float32) for p, kj in zip(ps, kjs)])
            acc[here, :] = alpha * acc[here, :] + pv

    def slot(i, _):
        base = pl.multiple_of(i * rows, rows)
        count = tbl[i * ROW]

        def key(n):
            return pl.multiple_of(tbl[i * ROW + 1 + n] * rows, rows)

        def two(n, _):
            update(base, [key(2 * n), key(2 * n + 1)])
            return 0

        lax.fori_loop(0, count // 2, two, 0)

        @pl.when(count % 2 == 1)
        def _():
            update(base, [key(count - 1)])

        return 0

    lax.fori_loop(0, n_q, slot, 0)

    if final:
        for j in range(4):
            here = pl.ds(pl.multiple_of(tbl[4 * ROW + j] * rows, rows), rows)
            total = jnp.sum(l_scr[here, :], axis=1, keepdims=True)
            o_out[j][...] = (acc[here, :] / total).astype(jnp.bfloat16)
    else:
        for i in range(n_q):
            for dst, src in zip(st_out[i], (acc, m_scr, l_scr)):
                dst[...] = src[at(i), :]


def attend(tbl, q_in, kv_in, keys, state, state_start, heads, final, hd, flops):
    first, count = heads
    rows = q_in[0].shape[0]
    n_q, n_state = len(q_in), len(state)
    scale = LOG2E * hd ** -0.5
    cfg = (n_q, n_state, tuple(keys), final, rows, scale)

    def spec(width, start):
        return pl.BlockSpec((rows, width), lambda h, t: (0, h + first - start))

    in_specs = [spec(hd, 0) for _ in q_in]
    in_specs += [spec(2 * hd, start) for _, start in kv_in]
    flat = [a for slot in state for a in slot]
    in_specs += [spec(hd, state_start) for _ in flat]
    if final:
        out_shape = [jax.ShapeDtypeStruct((rows, count * hd), jnp.bfloat16)] * 4
        out_specs = [pl.BlockSpec((rows, hd), lambda h, t: (0, h))] * 4
    else:
        out_shape = [jax.ShapeDtypeStruct((rows, count * hd), jnp.float32)] * (3 * n_q)
        out_specs = [pl.BlockSpec((rows, hd), lambda h, t: (0, h))] * (3 * n_q)
    outs = pl.pallas_call(
        functools.partial(attend_kernel, cfg),
        grid_spec=pltpu.PrefetchScalarGridSpec(
            num_scalar_prefetch=1,
            grid=(count,),
            in_specs=in_specs,
            out_specs=out_specs,
            scratch_shapes=[
                pltpu.VMEM((n_q * rows, hd), jnp.bfloat16),
                pltpu.VMEM((16 * rows, hd), jnp.bfloat16),
                pltpu.VMEM((16 * rows, hd), jnp.bfloat16),
            ] + [pltpu.VMEM((n_q * rows, hd), jnp.float32)] * 3,
        ),
        out_shape=out_shape,
        compiler_params=pltpu.CompilerParams(vmem_limit_bytes=60 * 2 ** 20),
        cost_estimate=pl.CostEstimate(flops=flops, bytes_accessed=2 ** 20, transcendentals=0),
    )(tbl, *q_in, *[a for a, _ in kv_in], *flat)
    if final:
        return list(outs)
    return [tuple(outs[3 * i:3 * i + 3]) for i in range(n_q)]


def out_kernel(n_groups, n_parts, tbl, *refs):
    o_in = refs[:4 * n_groups]
    w_in = refs[4 * n_groups:4 * n_groups + n_parts]
    y_ref, o_scr, w_scr, sem = refs[4 * n_groups + n_parts:]
    width, cols = o_in[0].shape[1], w_scr.shape[-1]
    copies = [pltpu.make_async_copy(w_in[s], w_scr.at[s], sem.at[s]) for s in range(n_parts)]
    for copy in copies:
        copy.start()
    for g in range(n_groups):
        for j in range(4):
            start = (j * n_groups + g) * width
            o_scr[:, start:start + width] = o_in[g * 4 + j][...]
    half = o_scr.shape[0] // 2
    for s in range(n_parts):
        copies[s].wait()
        there = pl.ds(pl.multiple_of(tbl[s] * cols, cols), cols)

        def rows_of(n, _):
            here = pl.ds(pl.multiple_of(n * half, half), half)
            y_ref[here, there] = jnp.dot(o_scr[here, :], w_scr[s], preferred_element_type=jnp.float32).astype(y_ref.dtype)
            return 0

        lax.fori_loop(0, 2, rows_of, 0)


def project_out(tbl, o_groups, w_parts):
    rows, _ = o_groups[0][0].shape
    depth, cols = w_parts[0].shape
    n_parts = len(w_parts)
    flat = [a for group in o_groups for a in group]
    return pl.pallas_call(
        functools.partial(out_kernel, len(o_groups), n_parts),
        in_specs=[pl.BlockSpec(memory_space=pltpu.SMEM)]
        + [pl.BlockSpec(memory_space=pltpu.VMEM) for _ in flat]
        + [pl.BlockSpec(memory_space=pl.ANY) for _ in w_parts],
        out_specs=pl.BlockSpec(memory_space=pltpu.VMEM),
        scratch_shapes=[
            pltpu.VMEM((rows, depth), jnp.bfloat16),
            pltpu.VMEM((n_parts, depth, cols), jnp.bfloat16),
            pltpu.SemaphoreType.DMA((n_parts,)),
        ],
        out_shape=jax.ShapeDtypeStruct((rows, n_parts * cols), jnp.bfloat16),
        compiler_params=pltpu.CompilerParams(vmem_limit_bytes=60 * 2 ** 20),
        cost_estimate=pl.CostEstimate(flops=2 * rows * depth * cols * n_parts, bytes_accessed=2 ** 24, transcendentals=0),
    )(tbl, *flat, *w_parts)


def solution(mesh):
    n_tp, n_cp = mesh.shape['tp'], mesh.shape['cp']
    make = work_tables(n_tp, n_cp)
    plans = [make(-1, 0), make(0, 1), make(1, 2), make(2, 3), make(1, 3)]

    def flip(axis, bit):
        n = mesh.shape[axis]
        return [(i, i ^ bit) for i in range(n)]

    def device_fn(x_loc, w_q, w_k, w_v, w_o):
        z, r = lax.axis_index('tp'), lax.axis_index('cp')
        d_model, n_heads, hd = w_q.shape
        inner = n_heads * hd
        ends = (z == 0) | (z == n_tp - 1)
        tables = [lax.dynamic_index_in_dim(jnp.asarray(p), z * n_cp + r, 0, keepdims=False) for p in plans]

        near = lax.ppermute(x_loc, 'tp', flip('tp', 1))
        mid = lax.ppermute(x_loc, 'tp', [(1, 2), (2, 1)])
        mid_out = lax.ppermute(mid, 'tp', [(1, 0), (2, 3)])
        far_mid = lax.ppermute(near, 'tp', [(1, 2), (2, 1)])
        far_out = lax.ppermute(far_mid, 'tp', [(1, 0), (2, 3)])

        wq = w_q.reshape(d_model, inner)
        wkv = jnp.concatenate([w_k, w_v], axis=2).reshape(d_model, 2 * inner)

        def project(xs, w):
            return jnp.dot(xs, w, preferred_element_type=jnp.float32).astype(jnp.bfloat16)

        def spread(kv):
            core = lax.ppermute(kv, 'cp', flip('cp', 1))
            chip = lax.ppermute(kv, 'cp', flip('cp', 2))
            both = lax.ppermute(chip, 'cp', flip('cp', 1))
            return [kv, core, chip, both]

        per = n_heads // GROUPS

        def spans(g):
            return slice(g * per * 2 * hd, (g + 1) * per * 2 * hd)

        def tie(value, *after):
            return lax.optimization_barrier((value,) + after)[0]

        q_steps, kv_all = [], {}

        def take(step, xs):
            for src, kv in enumerate(spread(project(xs, wkv))):
                kv_all[4 * step + src] = (kv, 0)
            q_steps.append(project(xs, wq))

        def pick(group, avail):
            return [kv_all[j] if j < 12 else kv_last[group][j] for j in avail]

        take(0, x_loc)
        take(1, near)
        first = attend(tables[0], q_steps[:2], pick(0, AVAIL[0]), AVAIL[0], [], 0, (0, n_heads), False, hd, 10 ** 9)
        take(2, jnp.where(ends, tie(mid_out, first[0][2]), mid))

        second = [None] * GROUPS

        def attend_second(g, tbl):
            second[g] = attend(tbl, q_steps[:3], pick(0, AVAIL[1]), AVAIL[1], first, 0, (g * per, per), False, hd, 10 ** 9)

        for g in range(GROUPS - 1):
            attend_second(g, tables[1])
        x_last = jnp.where(ends, tie(far_out, *[s[0][2] for s in second[:-1]]), far_mid)
        kv_last, own_last = [], []
        for g in range(GROUPS):
            kv = project(x_last, wkv[:, spans(g)])
            own_last.append(kv)
            kv_last.append({12 + src: (a, g * per) for src, a in enumerate(spread(kv))})
        q_steps.append(project(x_last, wq))
        attend_second(GROUPS - 1, tie(tables[1], *own_last, q_steps[3]))

        o_groups = []
        after = second[-1][0][2]
        for g in range(GROUPS):
            heads = (g * per, per)
            o_send = attend(tie(tables[4], after), q_steps, pick(g, AVAIL[3]), AVAIL[3], second[g], g * per, heads, True, hd, 3 * 10 ** 10)
            after = o_send[0]
            o_groups.append([o_send[0]] + [lax.ppermute(o_send[j], 'tp', flip('tp', j)) for j in range(1, 4)])

        dp = lax.axis_index('dp')
        quarter = 2 * dp + lax.rem(r, 2)
        cols = d_model // 4
        w_part = lax.dynamic_slice(w_o.reshape(inner, d_model), (0, quarter * cols), (inner, cols))
        w_part = tie(w_part, own_last[-1])
        w_got = [lax.ppermute(w_part, 'tp', flip('tp', j)) for j in range(1, 4)]
        w_mine = jnp.concatenate([w_part] + [tie(w, o_groups[0][0]) for w in w_got], axis=0)
        w_x = lax.ppermute(w_mine, 'dp', flip('dp', 1))
        w_all = [w_mine, w_x, lax.ppermute(w_mine, 'cp', flip('cp', 1)), lax.ppermute(tie(w_x, o_groups[-1][0]), 'cp', flip('cp', 1))]
        out_tbl = jnp.stack([quarter, quarter ^ 2, quarter ^ 1, quarter ^ 3]).astype(jnp.int32)
        return project_out(out_tbl, o_groups, w_all)

    seq_spec = P(('dp', 'cp', 'tp'), None)
    head_spec = P(None, 'tp', None)

    return jax.shard_map(device_fn, mesh=mesh, in_specs=(seq_spec, head_spec, head_spec, head_spec, P('tp', None, None)), out_specs=seq_spec, check_vma=False)
```

```python
import functools

import jax
import jax.numpy as jnp
import numpy as np
from jax import lax
from jax.experimental import pallas as pl
from jax.experimental.pallas import tpu as pltpu
from jax.sharding import PartitionSpec as P


LOG2E = 1.4426950408889634
ARRIVAL = ((0, 1, 2, 3), (1, 0, 2, 3), (2, 3, 1, 0), (3, 2, 1, 0))
HALF = 384
GROUPS = 3


def sub_block(run, rank, n_cp):
    if run < 2:
        return 2 * rank + run
    return 2 * (2 * n_cp - 1 - rank) + run - 2


LOCAL, REMOTE = (0, 1), (2, 3)


def key_slots(spec):
    return [4 * step + src for step, sources in spec for src in sources]


AVAIL = [
    key_slots([(0, LOCAL), (0, REMOTE), (1, LOCAL)]),
    key_slots([(0, LOCAL + REMOTE), (1, LOCAL + REMOTE), (2, LOCAL)]),
    key_slots([(0, LOCAL + REMOTE), (1, LOCAL + REMOTE), (2, LOCAL + REMOTE), (3, LOCAL)]),
    key_slots([(s, LOCAL + REMOTE) for s in range(4)]),
]
Q_SLOTS = [2, 3, 4, 4]
ROW = 20


def work_tables(n_tp, n_cp):
    def make(before, after):
        out = np.zeros((n_tp, n_cp, 5, ROW), np.int32)
        for z in range(n_tp):
            for r in range(n_cp):
                for i in range(Q_SLOTS[after]):
                    mine = sub_block(ARRIVAL[z][i], r, n_cp)
                    done = before >= 0 and i < Q_SLOTS[before]
                    keys = []
                    for j in AVAIL[after]:
                        if done and j in AVAIL[before]:
                            continue
                        other = sub_block(ARRIVAL[z][j // 4], r ^ (j % 4), n_cp)
                        if other < mine:
                            keys.append(j)
                    out[z, r, i, 0] = len(keys)
                    out[z, r, i, 1:1 + len(keys)] = keys
                order = (0, 1, 3, 2) if z in (1, 2) else (0, 1, 2, 3)
                out[z, r, 4, :4] = order
        return out.reshape(n_tp * n_cp, 5 * ROW)

    return make


def attend_kernel(cfg, tbl, *refs):
    (n_q, n_state, keys, final, rows, scale) = cfg
    refs = list(refs)
    q_in = [refs.pop(0) for _ in range(n_q)]
    kv_in = [refs.pop(0) for _ in keys]
    st_in = [[refs.pop(0) for _ in range(3)] for _ in range(n_state)]
    if final:
        o_out = [refs.pop(0) for _ in range(4)]
    else:
        st_out = [[refs.pop(0) for _ in range(3)] for _ in range(n_q)]
    q_scr, k_scr, v_scr, acc, m_scr, l_scr = refs
    hd = q_scr.shape[-1]

    def at(n):
        return pl.ds(n * rows, rows)

    for i in range(n_q):
        q_scr[at(i), :] = q_in[i][...]
    for j, ref in zip(keys, kv_in):
        k_scr[at(j), :] = ref[:, :hd]
        v_scr[at(j), :] = ref[:, hd:]
    for i in range(n_state):
        for dst, src in zip((acc, m_scr, l_scr), st_in[i]):
            dst[at(i), :] = src[...]

    def scores(q, kj, n):
        return lax.dot_general(q, k_scr[pl.ds(kj, n), :], (((1,), (1,)), ((), ())), preferred_element_type=jnp.float32)

    def lane_sums(p):
        out = p[:, :hd]
        for t in range(1, p.shape[1] // hd):
            out = out + p[:, t * hd:(t + 1) * hd]
        return out

    chunks = list(range(0, rows, HALF))

    for i in range(n_state, n_q):
        base = i * rows
        raws = [scores(q_scr[pl.ds(base + c, HALF), :], 4 * i * rows, c + HALF) for c in chunks]
        for c, s in zip(chunks, raws):
            n = c + HALF
            keep = lax.broadcasted_iota(jnp.int32, (HALF, n), 1) <= lax.broadcasted_iota(jnp.int32, (HALF, n), 0) + c
            s = jnp.where(keep, s * scale, -jnp.inf)
            m_new = jnp.broadcast_to(jnp.max(s, axis=1, keepdims=True), (HALF, hd))
            p = jnp.exp2(s - m_new[:, :1])
            here = pl.ds(base + c, HALF)
            l_scr[here, :] = lane_sums(p)
            m_scr[here, :] = m_new
            acc[here, :] = jnp.dot(p.astype(jnp.bfloat16), v_scr[pl.ds(4 * i * rows, n), :], preferred_element_type=jnp.float32)

    def update(base, kjs):
        def raw(c):
            q = q_scr[pl.ds(base + c, HALF), :]
            return [scores(q, kj, rows) for kj in kjs]

        nxt = raw(0)
        for n, c in enumerate(chunks):
            cur = nxt
            if n + 1 < len(chunks):
                nxt = raw(chunks[n + 1])
            here = pl.ds(base + c, HALF)
            m_old = m_scr[here, :]
            top = functools.reduce(jnp.maximum, cur)
            m_new = jnp.maximum(m_old, jnp.max(top, axis=1, keepdims=True) * scale)
            alpha = jnp.exp2(m_old - m_new)
            ps = [jnp.exp2(s * scale - m_new[:, :1]) for s in cur]
            sums = functools.reduce(jnp.add, [lane_sums(p) for p in ps])
            l_scr[here, :] = alpha * l_scr[here, :] + sums
            m_scr[here, :] = m_new
            pv = functools.reduce(jnp.add, [jnp.dot(p.astype(jnp.bfloat16), v_scr[pl.ds(kj, rows), :], preferred_element_type=jnp.float32) for p, kj in zip(ps, kjs)])
            acc[here, :] = alpha * acc[here, :] + pv

    def slot(i, _):
        base = pl.multiple_of(i * rows, rows)
        count = tbl[i * ROW]

        def key(n):
            return pl.multiple_of(tbl[i * ROW + 1 + n] * rows, rows)

        def two(n, _):
            update(base, [key(2 * n), key(2 * n + 1)])
            return 0

        lax.fori_loop(0, count // 2, two, 0)

        @pl.when(count % 2 == 1)
        def _():
            update(base, [key(count - 1)])

        return 0

    lax.fori_loop(0, n_q, slot, 0)

    if final:
        for j in range(4):
            here = pl.ds(pl.multiple_of(tbl[4 * ROW + j] * rows, rows), rows)
            total = jnp.sum(l_scr[here, :], axis=1, keepdims=True)
            o_out[j][...] = (acc[here, :] / total).astype(jnp.bfloat16)
    else:
        for i in range(n_q):
            for dst, src in zip(st_out[i], (acc, m_scr, l_scr)):
                dst[...] = src[at(i), :]


def attend(tbl, q_in, kv_in, keys, state, state_start, heads, final, hd, flops):
    first, count = heads
    rows = q_in[0].shape[0]
    n_q, n_state = len(q_in), len(state)
    scale = LOG2E * hd ** -0.5
    cfg = (n_q, n_state, tuple(keys), final, rows, scale)

    def spec(width, start):
        return pl.BlockSpec((rows, width), lambda h, t: (0, h + first - start))

    in_specs = [spec(hd, 0) for _ in q_in]
    in_specs += [spec(2 * hd, start) for _, start in kv_in]
    flat = [a for slot in state for a in slot]
    in_specs += [spec(hd, state_start) for _ in flat]
    if final:
        out_shape = [jax.ShapeDtypeStruct((rows, count * hd), jnp.bfloat16)] * 4
        out_specs = [pl.BlockSpec((rows, hd), lambda h, t: (0, h))] * 4
    else:
        out_shape = [jax.ShapeDtypeStruct((rows, count * hd), jnp.float32)] * (3 * n_q)
        out_specs = [pl.BlockSpec((rows, hd), lambda h, t: (0, h))] * (3 * n_q)
    outs = pl.pallas_call(
        functools.partial(attend_kernel, cfg),
        grid_spec=pltpu.PrefetchScalarGridSpec(
            num_scalar_prefetch=1,
            grid=(count,),
            in_specs=in_specs,
            out_specs=out_specs,
            scratch_shapes=[
                pltpu.VMEM((n_q * rows, hd), jnp.bfloat16),
                pltpu.VMEM((16 * rows, hd), jnp.bfloat16),
                pltpu.VMEM((16 * rows, hd), jnp.bfloat16),
            ] + [pltpu.VMEM((n_q * rows, hd), jnp.float32)] * 3,
        ),
        out_shape=out_shape,
        compiler_params=pltpu.CompilerParams(vmem_limit_bytes=60 * 2 ** 20),
        cost_estimate=pl.CostEstimate(flops=flops, bytes_accessed=2 ** 20, transcendentals=0),
    )(tbl, *q_in, *[a for a, _ in kv_in], *flat)
    if final:
        return list(outs)
    return [tuple(outs[3 * i:3 * i + 3]) for i in range(n_q)]


def out_kernel(n_groups, n_parts, tbl, *refs):
    o_in = refs[:4 * n_groups]
    w_in = refs[4 * n_groups:4 * n_groups + n_parts]
    y_ref, o_scr, w_scr, sem = refs[4 * n_groups + n_parts:]
    width, cols = o_in[0].shape[1], w_scr.shape[-1]
    copies = [pltpu.make_async_copy(w_in[s], w_scr.at[s], sem.at[s]) for s in range(n_parts)]
    for copy in copies:
        copy.start()
    for g in range(n_groups):
        for j in range(4):
            start = (j * n_groups + g) * width
            o_scr[:, start:start + width] = o_in[g * 4 + j][...]
    half = o_scr.shape[0] // 2
    for s in range(n_parts):
        copies[s].wait()
        there = pl.ds(pl.multiple_of(tbl[s] * cols, cols), cols)

        def rows_of(n, _):
            here = pl.ds(pl.multiple_of(n * half, half), half)
            y_ref[here, there] = jnp.dot(o_scr[here, :], w_scr[s], preferred_element_type=jnp.float32).astype(y_ref.dtype)
            return 0

        lax.fori_loop(0, 2, rows_of, 0)


def project_out(tbl, o_groups, w_parts):
    rows, _ = o_groups[0][0].shape
    depth, cols = w_parts[0].shape
    n_parts = len(w_parts)
    flat = [a for group in o_groups for a in group]
    return pl.pallas_call(
        functools.partial(out_kernel, len(o_groups), n_parts),
        in_specs=[pl.BlockSpec(memory_space=pltpu.SMEM)]
        + [pl.BlockSpec(memory_space=pltpu.VMEM) for _ in flat]
        + [pl.BlockSpec(memory_space=pl.ANY) for _ in w_parts],
        out_specs=pl.BlockSpec(memory_space=pltpu.VMEM),
        scratch_shapes=[
            pltpu.VMEM((rows, depth), jnp.bfloat16),
            pltpu.VMEM((n_parts, depth, cols), jnp.bfloat16),
            pltpu.SemaphoreType.DMA((n_parts,)),
        ],
        out_shape=jax.ShapeDtypeStruct((rows, n_parts * cols), jnp.bfloat16),
        compiler_params=pltpu.CompilerParams(vmem_limit_bytes=60 * 2 ** 20),
        cost_estimate=pl.CostEstimate(flops=2 * rows * depth * cols * n_parts, bytes_accessed=2 ** 24, transcendentals=0),
    )(tbl, *flat, *w_parts)


def solution(mesh):
    n_tp, n_cp = mesh.shape['tp'], mesh.shape['cp']
    make = work_tables(n_tp, n_cp)
    plans = [make(-1, 0), make(0, 1), make(1, 2), make(2, 3), make(1, 3)]

    def flip(axis, bit):
        n = mesh.shape[axis]
        return [(i, i ^ bit) for i in range(n)]

    def device_fn(x_loc, w_q, w_k, w_v, w_o):
        z, r = lax.axis_index('tp'), lax.axis_index('cp')
        d_model, n_heads, hd = w_q.shape
        inner = n_heads * hd
        ends = (z == 0) | (z == n_tp - 1)
        tables = [lax.dynamic_index_in_dim(jnp.asarray(p), z * n_cp + r, 0, keepdims=False) for p in plans]

        near = lax.ppermute(x_loc, 'tp', flip('tp', 1))
        mid = lax.ppermute(x_loc, 'tp', [(1, 2), (2, 1)])
        mid_out = lax.ppermute(mid, 'tp', [(1, 0), (2, 3)])
        far_mid = lax.ppermute(near, 'tp', [(1, 2), (2, 1)])
        far_out = lax.ppermute(far_mid, 'tp', [(1, 0), (2, 3)])

        wq = w_q.reshape(d_model, inner)
        wkv = jnp.concatenate([w_k, w_v], axis=2).reshape(d_model, 2 * inner)

        def project(xs, w):
            return jnp.dot(xs, w, preferred_element_type=jnp.float32).astype(jnp.bfloat16)

        def spread(kv):
            core = lax.ppermute(kv, 'cp', flip('cp', 1))
            chip = lax.ppermute(kv, 'cp', flip('cp', 2))
            both = lax.ppermute(chip, 'cp', flip('cp', 1))
            return [kv, core, chip, both]

        per = n_heads // GROUPS

        def spans(g):
            return slice(g * per * 2 * hd, (g + 1) * per * 2 * hd)

        def tie(value, *after):
            return lax.optimization_barrier((value,) + after)[0]

        q_steps, kv_all = [], {}

        def take(step, xs):
            for src, kv in enumerate(spread(project(xs, wkv))):
                kv_all[4 * step + src] = (kv, 0)
            q_steps.append(project(xs, wq))

        def pick(group, avail):
            return [kv_all[j] if j < 12 else kv_last[group][j] for j in avail]

        take(0, x_loc)
        take(1, near)
        first = attend(tables[0], q_steps[:2], pick(0, AVAIL[0]), AVAIL[0], [], 0, (0, n_heads), False, hd, 10 ** 9)
        take(2, jnp.where(ends, tie(mid_out, first[0][2]), mid))

        second = [None] * GROUPS

        def attend_second(g, tbl):
            second[g] = attend(tbl, q_steps[:3], pick(0, AVAIL[1]), AVAIL[1], first, 0, (g * per, per), False, hd, 10 ** 9)

        attend_second(0, tables[1])
        x_last = jnp.where(ends, tie(far_out, second[0][0][2]), far_mid)
        kv_last, own_last = [], []
        for g in range(GROUPS):
            kv = project(x_last, wkv[:, spans(g)])
            own_last.append(kv)
            kv_last.append({12 + src: (a, g * per) for src, a in enumerate(spread(kv))})
        q_steps.append(project(x_last, wq))
        behind = [*own_last, q_steps[3]]
        for g in range(1, GROUPS):
            attend_second(g, tie(tables[1], *behind))
            behind = [second[g][0][2]]

        o_groups = []
        after = second[-1][0][2]
        for g in range(GROUPS):
            heads = (g * per, per)
            o_send = attend(tie(tables[4], after), q_steps, pick(g, AVAIL[3]), AVAIL[3], second[g], g * per, heads, True, hd, 3 * 10 ** 10)
            after = o_send[0]
            o_groups.append([o_send[0]] + [lax.ppermute(o_send[j], 'tp', flip('tp', j)) for j in range(1, 4)])

        dp = lax.axis_index('dp')
        quarter = 2 * dp + lax.rem(r, 2)
        cols = d_model // 4
        w_part = lax.dynamic_slice(w_o.reshape(inner, d_model), (0, quarter * cols), (inner, cols))
        w_part = tie(w_part, own_last[-1])
        w_got = [lax.ppermute(w_part, 'tp', flip('tp', j)) for j in range(1, 4)]
        w_mine = jnp.concatenate([w_part] + [tie(w, o_groups[0][0]) for w in w_got], axis=0)
        w_x = lax.ppermute(w_mine, 'dp', flip('dp', 1))
        w_all = [w_mine, w_x, lax.ppermute(w_mine, 'cp', flip('cp', 1)), lax.ppermute(tie(w_x, o_groups[-1][0]), 'cp', flip('cp', 1))]
        out_tbl = jnp.stack([quarter, quarter ^ 2, quarter ^ 1, quarter ^ 3]).astype(jnp.int32)
        return project_out(out_tbl, o_groups, w_all)

    seq_spec = P(('dp', 'cp', 'tp'), None)
    head_spec = P(None, 'tp', None)

    return jax.shard_map(device_fn, mesh=mesh, in_specs=(seq_spec, head_spec, head_spec, head_spec, P('tp', None, None)), out_specs=seq_spec, check_vma=False)
```
